32 devices in a mesh: section: 4 (over x, core), tensor: 8 (over z, y).
Axes of the slice: x: 2, y: 2, z: 4, core: 2. Of those that a mesh axis runs over, the one named last changes fastest.
Arguments:
- tokens: bfloat16 [2, 64, 4096], replicated, may hold values from -6 to 6
- norm_gain: bfloat16 [4, 4096], replicated, may hold values from 0.25 to 1.75
- w_in: bfloat16 [4, 2, 14336, 4096], P('section', None, 'tensor'), may hold values from -0.09375 to 0.09375
- w_out: bfloat16 [4, 14336, 4096], P('section', 'tensor'), may hold values from -0.046875 to 0.046875
- backup_in: bfloat16 [4, 2, 14336, 4096], P('section', None, 'tensor'), may hold values from -0.09375 to 0.09375
- backup_out: bfloat16 [4, 14336, 4096], P('section', None, 'tensor'), may hold values from -0.046875 to 0.046875
- layer_group: int32 [4], replicated, may hold values from 0 to 3, as said below
- token_counts: int32 [2], replicated, may hold values from 1 to 64, as said below
Outputs:
- handed: bfloat16 [4, 2, 64, 4096], P('section', None, 'tensor')
The draws below stay inside these ranges and needn't reach their ends.
Inputs may be any that keep to these rules, and one draw needn't show every extreme that they name: layer_group[l] is l or l + 1. The layers that move up form one run of consecutive layers, at least one, that starts at the layer of the one group left without any layer; that group is never the last one. `token_counts`: rows of a micro-batch from its count on are padding. One micro-batch is full, with 64 real tokens; the other has at most 32.
All inputs are finite; a program needn't handle non-finite values.
Results may differ from the reference program's by a relative error of at most 0.025.
Values may be sent and summed in bfloat16 or wider, within the bound.
A program may use at most 192 MiB of HBM per device.

```python
import jax
import jax.numpy as jnp
from jax import lax

D = 4096
FF = 14336
TOK = 64
MB = 2
LAYERS = 4
BLOCKS = 8


def draw_layer_group(key, part):
    key_lost, key_span = jax.random.split(jax.random.fold_in(key, 7))
    lost_group = jax.random.randint(key_lost, (), 0, LAYERS - 1)
    span_count = 1 + jax.random.randint(key_span, (), 0, LAYERS - 1 - lost_group)
    levels = jnp.arange(LAYERS, dtype=jnp.int32)
    moved_up = (levels >= lost_group) & (levels < lost_group + span_count)
    return levels + moved_up.astype(jnp.int32)


def draw_token_counts(key, part):
    key_low, key_flip = jax.random.split(jax.random.fold_in(key, 11))
    high_count = jnp.int32(TOK)
    low_count = jax.random.randint(key_low, (), 1, TOK // 2 + 1)
    flipped = jax.random.randint(key_flip, (), 0, 2)
    first = jnp.where(flipped == 1, low_count, high_count)
    second = jnp.where(flipped == 1, high_count, low_count)
    return jnp.stack([first, second]).astype(jnp.int32)


def block_levels(key, shape, cuts, smallest, high):
    gain, own = 1.0, jax.random.fold_in(key, 6)
    for dim, parts in cuts:
        steps = jnp.exp(jax.random.uniform(jax.random.fold_in(own, dim), (parts,), jnp.float32, smallest / len(cuts), high / len(cuts)))
        gain = gain * jnp.repeat(steps, shape[dim] // parts).reshape([-1 if axis == dim else 1 for axis in range(len(shape))])
    return gain


def gaussian(stream_key, extent, scale, reach, cuts=(), kind=jnp.bfloat16):
    result = jax.random.normal(stream_key, extent, jnp.float32) * scale
    if len(cuts) > 0:
        result = block_levels(stream_key, extent, cuts, -0.22, 0.18) * result
    return jnp.clip(result, min=-reach, max=reach).astype(kind)


def setup_inputs(seed: int = 0) -> dict:
    splits = jax.random.split(jax.random.key(seed), 9)
    tokens = gaussian(splits[0], (MB, TOK, D), 1.0, 6.0)
    norm_gain = jnp.clip(1.0 + 0.15 * jax.random.normal(splits[1], (LAYERS, D), jnp.float32), 0.25, 1.75).astype(jnp.bfloat16)
    w_in = gaussian(splits[2], (LAYERS, 2, FF, D), D ** -0.5, 0.09375, ((0, 4), (2, 8)))
    w_out = gaussian(splits[3], (LAYERS, FF, D), FF ** -0.5, 0.046875, ((0, 4), (1, 8)))
    backup_in = gaussian(splits[4], (LAYERS, 2, FF, D), D ** -0.5, 0.09375, ((0, 4), (2, 8)))
    backup_out = gaussian(splits[5], (LAYERS, FF, D), FF ** -0.5, 0.046875, ((0, 4), (2, 8)))
    layer_group = draw_layer_group(jax.random.fold_in(splits[8], 71), 0)
    token_counts = draw_token_counts(jax.random.fold_in(splits[8], 71), 0)
    return {"tokens": tokens, "norm_gain": norm_gain, "w_in": w_in, "w_out": w_out, "backup_in": backup_in, "backup_out": backup_out, "layer_group": layer_group, "token_counts": token_counts}


NORM_EPS = 0.25

def apply_layer(current, gain_row, w_pair, w_down, row_keep):
    wide_x = current.astype(jnp.float32)
    mean_square = lax.optimization_barrier(jnp.mean(wide_x * wide_x, axis=1, keepdims=True))
    normed = (wide_x * lax.rsqrt(mean_square + NORM_EPS) * gain_row.astype(jnp.float32)).astype(jnp.bfloat16)
    gate_part = lax.dot_general(normed, w_pair[0], (((1,), (1,)), ((), ())), preferred_element_type=jnp.float32)
    up_part = lax.dot_general(normed, w_pair[1], (((1,), (1,)), ((), ())), preferred_element_type=jnp.float32)
    hidden = (jax.nn.silu(gate_part) * up_part).astype(jnp.bfloat16)
    row_count = hidden.shape[0]
    block_width = FF // BLOCKS
    hidden_blocks = hidden.reshape(row_count, BLOCKS, block_width).astype(jnp.float32)
    down_blocks = w_down.reshape(BLOCKS, block_width, D).astype(jnp.float32)
    partial_value = jnp.einsum('rbf,bfd->brd', hidden_blocks, down_blocks)
    rounded = lax.optimization_barrier(partial_value.astype(jnp.bfloat16))
    summed = lax.optimization_barrier(jnp.sum(rounded.astype(jnp.float32), axis=0))
    return (wide_x + row_keep * summed).astype(jnp.bfloat16)

def reference(tokens, norm_gain, w_in, w_out, backup_in, backup_out, layer_group, token_counts):
    positions = jnp.arange(TOK, dtype=jnp.int32)
    row_keep = (positions[None, :] < token_counts[:, None]).astype(jnp.float32).reshape(MB * TOK, 1)
    current = tokens.reshape(MB * TOK, D)
    history = [current]
    for level in range(LAYERS):
        moved = layer_group[level] == level + 1
        spare = (level + 1) % LAYERS
        pair = jnp.where(moved, backup_in[spare], w_in[level])
        down = jnp.where(moved, backup_out[spare], w_out[level])
        current = apply_layer(current, norm_gain[level][None, :], pair, down, row_keep)
        history.append(current)
    stacked = jnp.stack(history).reshape(LAYERS + 1, MB, TOK, D)
    groups = jnp.arange(LAYERS, dtype=jnp.int32)
    reached = lax.optimization_barrier(jnp.sum((layer_group[None, :] <= groups[:, None]).astype(jnp.int32), axis=1))
    return jnp.take(stacked, reached, axis=0)
```

```python
import functools

import jax
import jax.numpy as jnp
from jax import lax
from jax.experimental import pallas as pl
from jax.experimental.pallas import tpu as pltpu
from jax.sharding import PartitionSpec as P

NORM_EPS = 0.25
MESH = pl.DeviceIdType.MESH
F32 = jnp.float32
BF16 = jnp.bfloat16


def as_int(condition):
    return jnp.where(condition, 1, 0)


def relay_kernel(
    cfg, counts, tokens_hbm, gain_hbm, w_in, w_out, b_in, b_out, out,
    wi, wo, xs, acc, hid, hidp, psum, rsum, ssum, res, xblk, psum2, rsum2, row_out, row_in, tok, tsel, gain, gain_row, ssq,
    wi_sem, wo_sem, in_sem, ag_recv, own_send, fwd_send, h_recv, h_own, h_fwd,
    rs_send, rs_recv, res_sem, xb_sem, rs2_send, rs2_recv, row_send, row_recv,
):
    lost, span, sections, layers, n, tok_rows, features, units, pieces = cfg
    half = tok_rows // 2
    rows = tok_rows + half
    share = tok_rows // n
    width = features // n
    lines = n // 2
    piece = units // pieces
    group = lax.axis_index("section")
    me = lax.axis_index("tensor")
    line = me // 2
    side = lax.rem(me, 2)

    def moved(level):
        return (level >= lost) & (level < lost + span)

    def owner(level):
        return level + as_int(moved(level))

    def near(i):
        edge = jnp.minimum(line, lines - 1 - line)
        alternate = jnp.where(lax.rem(i, 2) == 1, line + (i + 1) // 2, line - i // 2)
        beyond = jnp.where(line < lines - 1 - line, i, lines - 1 - i)
        return jnp.where(i <= 2 * edge, alternate, beyond)

    def row_slot(i):
        return 2 * near(i) + side

    def across_slot(i):
        return 2 * near(i) + 1 - side

    def step_slot(s):
        across = (s > 0) & ((lax.rem(s, 2) == 0) | (s == n - 1))
        i = jnp.where(s == n - 1, lines - 1, jnp.where(across, s // 2 - 1, (s + 1) // 2))
        return across, i, 2 * near(i) + jnp.where(across, 1 - side, side)

    def columns(slot):
        return pl.ds(pl.multiple_of(slot * width, 128), width)

    def load_in(src, slot):
        return pltpu.make_async_copy(src.at[0, :, :, columns(slot)], wi.at[slot], wi_sem.at[slot])

    def load_out_own(slot):
        return pltpu.make_async_copy(w_out.at[0, :, columns(slot)], wo.at[slot], wo_sem.at[slot])

    def load_out_backup(slot):
        start = pl.multiple_of(slot * units, 64)
        return pltpu.make_async_copy(b_out.at[0, pl.ds(start, units), :], wo.at[slot], wo_sem.at[slot])

    def each(count, body):
        def step(i, carry):
            body(i)
            return carry

        lax.fori_loop(0, count, step, 0)

    def start_in(src):
        each(n, lambda s: load_in(src, step_slot(s)[2]).start())

    barrier = pltpu.get_barrier_semaphore()

    def greet(o):
        target = (lax.rem(group + o // n, sections), lax.rem(me + lax.rem(o, n), n))
        pl.semaphore_signal(barrier, inc=1, device_id=target, device_id_type=MESH)

    each(sections * n - 1, lambda o: greet(o + 1))
    fetch_tok = pltpu.make_async_copy(tokens_hbm, tok, in_sem.at[0])
    fetch_gain = pltpu.make_async_copy(gain_hbm, gain, in_sem.at[1])
    fetch_tok.start()
    fetch_gain.start()
    has_backup = (group > lost) & (group <= lost + span)
    has_own = (group < lost) | (group >= lost + span)
    double = group == lost + span

    @pl.when(has_backup)
    def _():
        start_in(b_in)
        each(n, lambda s: load_out_backup(step_slot(s)[2]).start())

    @pl.when(has_own & jnp.logical_not(has_backup))
    def _():
        start_in(w_in)
        each(n, lambda s: load_out_own(step_slot(s)[2]).start())

    fetch_tok.wait()
    fetch_gain.wait()
    full_second = counts[1] > counts[0]
    part_count = jnp.minimum(counts[0], counts[1])
    row_ids = lax.broadcasted_iota(jnp.int32, (rows, 1), 0)
    keep = ((row_ids < tok_rows) | (row_ids - tok_rows < part_count)).astype(F32)

    def pick_tokens(mb, cols):
        return jnp.where(full_second, tok[1 - mb, :, cols], tok[mb, :, cols])

    pick = (
        lax.broadcasted_iota(jnp.int32, (8, tok_rows), 1)
        == me * share + lax.broadcasted_iota(jnp.int32, (8, tok_rows), 0)
    ).astype(BF16)

    def keep_tokens(c):
        for mb in range(2):
            chosen = jnp.dot(pick, pick_tokens(mb, columns(c)), preferred_element_type=F32)
            tsel[mb, :, columns(c)] = chosen.astype(BF16)

        @pl.when(group == owner(0))
        def _():
            xs[0, c, :tok_rows] = pick_tokens(0, columns(c))
            xs[0, c, tok_rows:] = pick_tokens(1, columns(c))[:half]

    each(n, keep_tokens)

    pl.semaphore_wait(barrier, sections * n - 1)

    def remote(src, dst, send, recv, device):
        return pltpu.make_async_remote_copy(
            src_ref=src, dst_ref=dst, send_sem=send, recv_sem=recv, device_id=device, device_id_type=MESH
        )

    across_peer = (group, 2 * line + 1 - side)

    def ag_copy(par, slot, send, device):
        return remote(xs.at[par, slot], xs.at[par, slot], send, ag_recv.at[par, slot], device)

    def h_copy(slot, p, send, device):
        return remote(hid.at[slot, p], hid.at[slot, p], send, h_recv.at[slot, p], device)

    def rs_copy(target_group, target):
        return remote(
            psum.at[target], rsum.at[me], rs_send.at[target], rs_recv.at[me], (target_group, target)
        )

    def res_copy(par, target_group):
        return remote(xs.at[par, me], res, res_sem.at[0], res_sem.at[1], (target_group, me))

    def xb_copy(target_group):
        return remote(xblk, xblk, xb_sem.at[0], xb_sem.at[1], (target_group, me))

    def rs2_copy(target, c):
        return remote(
            psum2.at[target, c],
            rsum2.at[me, c],
            rs2_send.at[target, c],
            rs2_recv.at[me, c],
            (group, target),
        )

    def rs2_arrival(source, c):
        return remote(
            psum2.at[me, c],
            rsum2.at[source, c],
            rs2_send.at[me, c],
            rs2_recv.at[source, c],
            (group, source),
        )

    def row_copy(i, target_group):
        return remote(row_out, row_in, row_send.at[i], row_recv, (target_group, me))

    def row_choice(count):
        r = lax.broadcasted_iota(jnp.int32, (16, count), 0)
        c = lax.broadcasted_iota(jnp.int32, (16, count), 1)
        inner = lax.rem(r, 8)
        row = me * share + inner
        full = (r < 8) & (c == row)
        part = (r >= 8) & (c == row + tok_rows) & (row < half)
        return ((inner < share) & (full | part)).astype(BF16)

    def level_body(level):
        par = lax.rem(level, 2)
        home = owner(jnp.minimum(level + 1, layers - 1))
        first = level == 0
        last = level == layers - 1
        before = owner(jnp.maximum(level - 1, 0))
        is_moved = moved(level)
        before_moved = moved(level - 1)

        @pl.when(jnp.logical_not(first) & jnp.logical_not(before_moved))
        def _():
            res_copy(par, group).wait_recv()
            for j in range(n):
                remote(psum.at[0], rsum.at[j], rs_send.at[0], rs_recv.at[j], (group, me)).wait_recv()
            total = rsum[0].astype(F32)
            for j in range(1, n):
                total = total + rsum[j].astype(F32)
            xs[par, me] = (res[...].astype(F32) + keep * total).astype(BF16)

        @pl.when(jnp.logical_not(first) & before_moved)
        def _():
            @pl.when(before != group)
            def _():
                xb_copy(group).wait_recv()

            xs[par, me] = xblk[...]

        @pl.when(jnp.logical_not(first))
        def _():
            ag_copy(par, me, own_send.at[0], across_peer).start()
            each(
                lines - 1,
                lambda i: ag_copy(par, me, own_send.at[i + 1], (group, row_slot(i + 1))).start(),
            )

        @pl.when(jnp.logical_not(last) & jnp.logical_not(is_moved))
        def _():
            res_copy(par, home).start()

        acc[...] = jnp.zeros_like(acc)
        ssq[...] = jnp.zeros_like(ssq)
        for index in range(layers):

            @pl.when(level == index)
            def _():
                gain_row[...] = gain[index : index + 1].astype(F32)


        def chunk(s):
            across, i, slot = step_slot(s)

            @pl.when(jnp.logical_not(first) & (s > 0))
            def _():
                ag_copy(par, slot, own_send.at[0], across_peer).wait_recv()

            @pl.when(jnp.logical_not(first) & (s > 0) & jnp.logical_not(across))
            def _():
                ag_copy(par, slot, fwd_send.at[i], across_peer).start()

            load_in(w_in, slot).wait()
            wide = xs[par, slot].astype(F32)
            square = wide * wide
            lane = square[:, :128]
            for q in range(1, width // 128):
                lane = lane + square[:, q * 128 : (q + 1) * 128]
            ssq[...] += lane
            scaled = (wide * gain_row[:, columns(slot)]).astype(BF16)
            for p in range(pieces):
                for half_id in range(2):
                    acc[half_id, p] += lax.dot_general(
                        scaled,
                        wi[slot, half_id, p * piece : (p + 1) * piece],
                        (((1,), (1,)), ((), ())),
                        preferred_element_type=F32,
                    )

        each(n, chunk)

        @pl.when(double & is_moved)
        def _():
            start_in(w_in)

        mean_square = jnp.sum(ssq[...], axis=1, keepdims=True) * (1.0 / features)
        scale = lax.rsqrt(mean_square + NORM_EPS)

        def hidden(p):
            gate = acc[0, p] * scale
            up = acc[1, p] * scale
            return (gate / (1.0 + jnp.exp(-gate)) * up).astype(BF16)

        def down(source, weights):
            total = jnp.dot(source[0], wo[weights, :piece], preferred_element_type=F32)
            for p in range(1, pieces):
                total = total + jnp.dot(
                    source[p], wo[weights, p * piece : (p + 1) * piece], preferred_element_type=F32
                )
            return total

        @pl.when(is_moved)
        def _():
            def produce(p):
                hid[me, p] = hidden(p)
                h_copy(me, p, h_own.at[0, p], across_peer).start()
                h_copy(me, p, h_own.at[1, p], (group, row_slot(1))).start()

            each(pieces, produce)

            def send_far(i):
                each(
                    pieces,
                    lambda p: h_copy(me, p, h_own.at[i, p], (group, row_slot(i))).start(),
                )

            each(lines - 2, lambda i: send_far(i + 2))

            def contribution(slot):
                load_out_own(slot).wait()
                return down(hid.at[slot], slot).astype(BF16).astype(F32)

            ssum[...] = contribution(me)

            def gather(i):
                @pl.when(i < lines)
                def _():
                    slot = row_slot(i)

                    def pass_on(p):
                        h_copy(slot, p, h_own.at[0, p], across_peer).wait_recv()
                        h_copy(slot, p, h_fwd.at[i, p], across_peer).start()

                    each(pieces, pass_on)
                    ssum[...] += contribution(slot)

                other = across_slot(i - 1)
                each(pieces, lambda p: h_copy(other, p, h_own.at[0, p], across_peer).wait_recv())
                ssum[...] += contribution(other)

            each(lines, lambda i: gather(i + 1))
            xblk[...] = (xs[par, me].astype(F32) + keep * ssum[...]).astype(BF16)

            @pl.when(home != group)
            def _():
                xb_copy(home).start()

            @pl.when(double)
            def _():
                each(n, lambda s: load_out_own(step_slot(s)[2]).start())

        @pl.when(jnp.logical_not(is_moved) & jnp.logical_not(last))
        def _():
            def produce(p):
                hid[me, p] = hidden(p)

            each(pieces, produce)

            def reduce_block(s):
                slot = step_slot(n - 1 - s)[2]
                load_out_own(slot).wait()
                psum[slot] = down(hid.at[me], slot).astype(BF16)
                rs_copy(home, slot).start()

            each(n, reduce_block)

        @pl.when(last)
        def _():
            r = lax.broadcasted_iota(jnp.int32, (n * 16, rows), 0)
            c = lax.broadcasted_iota(jnp.int32, (n * 16, rows), 1)
            inner = lax.rem(r, 8)
            row = (r // 16) * share + inner
            is_full = lax.rem(r, 16) < 8
            target_row = jnp.where(is_full, row, row + tok_rows)
            valid = (inner < share) & (is_full | (row < half))
            order = (valid & (c == target_row)).astype(BF16)

            def produce(p):
                hidp[p] = jnp.dot(order, hidden(p), preferred_element_type=F32).astype(BF16)

            each(pieces, produce)

            def reduce_rows(c):
                load_out_own(c).wait()
                total = down(hidp, c).astype(BF16)
                for j in range(n):
                    psum2[j, c] = total[16 * j : 16 * (j + 1)]
                rsum2[me, c] = psum2[me, c]
                each(n - 1, lambda o: rs2_copy(lax.rem(me + o + 1, n), c).start())

            each(n, reduce_rows)

        hand_before = jnp.logical_not(first) & (before != group)
        hand_lost = jnp.logical_not(first) & (level == lost)
        choice = row_choice(rows)

        @pl.when(hand_before | hand_lost)
        def _():
            def choose(c):
                chosen = jnp.dot(choice, xs[par, c], preferred_element_type=F32)
                row_out[:, columns(c)] = chosen.astype(BF16)

            each(n, choose)

        @pl.when(hand_before)
        def _():
            row_copy(0, before).start()

        @pl.when(hand_lost)
        def _():
            row_copy(1, lost).start()

        @pl.when(last)
        def _():
            r = lax.broadcasted_iota(jnp.int32, (16, 1), 0)
            kept = ((r < 8) | (me * share + r - 8 < part_count)).astype(F32)

            def finish(c):
                each(n - 1, lambda o: rs2_arrival(lax.rem(me + o + 1, n), c).wait_recv())
                total = rsum2[0, c].astype(F32)
                for j in range(1, n):
                    total = total + rsum2[j, c].astype(F32)
                entered = jnp.dot(choice, xs[par, c], preferred_element_type=F32)
                row_in[:, columns(c)] = (entered + kept * total).astype(BF16)

            each(n, finish)

        @pl.when(jnp.logical_not(first))
        def _():
            each(lines, lambda i: ag_copy(par, me, own_send.at[i], across_peer).wait_send())
            each(lines - 1, lambda i: ag_copy(par, me, fwd_send.at[i + 1], across_peer).wait_send())

        @pl.when(is_moved)
        def _():
            for i in range(lines):
                each(pieces, lambda p: h_copy(me, p, h_own.at[i, p], across_peer).wait_send())
            for i in range(1, lines):
                each(pieces, lambda p: h_copy(me, p, h_fwd.at[i, p], across_peer).wait_send())

            @pl.when(home != group)
            def _():
                xb_copy(home).wait_send()

        @pl.when(jnp.logical_not(is_moved) & jnp.logical_not(last))
        def _():
            res_copy(par, home).wait_send()
            each(n, lambda s: rs_copy(home, s).wait_send())

        @pl.when(last)
        def _():
            each(n, lambda c: each(n - 1, lambda o: rs2_copy(lax.rem(me + o + 1, n), c).wait_send()))

        @pl.when(hand_before)
        def _():
            row_copy(0, before).wait_send()

        @pl.when(hand_lost)
        def _():
            row_copy(1, lost).wait_send()

    def level(l):
        @pl.when(group == owner(l))
        def _():
            level_body(l)

    each(layers, level)

    untouched = (lost == 0) & (group == 0)

    @pl.when(jnp.logical_not(untouched) & (group != sections - 1))
    def _():
        row_copy(0, group).wait_recv()

    @pl.when(untouched)
    def _():
        row_in[:8] = tsel[0]
        row_in[8:] = tsel[1]

    r = lax.broadcasted_iota(jnp.int32, (8, 1), 0)
    full_rows = row_in[:8]
    part_rows = jnp.where(me * share + r < half, row_in[8:], tsel[1])
    out[0, 0] = jnp.where(full_second, part_rows, full_rows)[:share]
    out[0, 1] = jnp.where(full_second, full_rows, part_rows)[:share]


def run_plan(
    plan, channel, n, sections, tokens, norm_gain, w_in, w_out, backup_in, backup_out, token_counts
):
    _, tok_rows, features = tokens.shape
    layers = norm_gain.shape[0]
    units = w_in.shape[2]
    piece = next((size for size in (256, 128) if units % size == 0), units)
    pieces = units // piece
    rows = tok_rows + tok_rows // 2
    width = features // n
    lines = n // 2
    cfg = plan + (sections, layers, n, tok_rows, features, units, pieces)
    anywhere = pl.BlockSpec(memory_space=pl.ANY)
    dma = pltpu.SemaphoreType.DMA
    return pl.pallas_call(
        functools.partial(relay_kernel, cfg),
        out_shape=jax.ShapeDtypeStruct((1, 2, tok_rows // n, features), BF16),
        in_specs=[pl.BlockSpec(memory_space=pltpu.SMEM)] + [anywhere] * 6,
        out_specs=pl.BlockSpec(memory_space=pltpu.VMEM),
        scratch_shapes=[
            pltpu.VMEM((n, 2, units, width), BF16),
            pltpu.VMEM((n, units, width), BF16),
            pltpu.VMEM((2, n, rows, width), BF16),
            pltpu.VMEM((2, pieces, rows, piece), F32),
            pltpu.VMEM((n, pieces, rows, piece), BF16),
            pltpu.VMEM((pieces, n * 16, piece), BF16),
            pltpu.VMEM((n, rows, width), BF16),
            pltpu.VMEM((n, rows, width), BF16),
            pltpu.VMEM((rows, width), F32),
            pltpu.VMEM((rows, width), BF16),
            pltpu.VMEM((rows, width), BF16),
            pltpu.VMEM((n, n, 16, width), BF16),
            pltpu.VMEM((n, n, 16, width), BF16),
            pltpu.VMEM((16, features), BF16),
            pltpu.VMEM((16, features), BF16),
            pltpu.VMEM((2, tok_rows, features), BF16),
            pltpu.VMEM((2, 8, features), BF16),
            pltpu.VMEM((layers, features), BF16),
            pltpu.VMEM((1, features), F32),
            pltpu.VMEM((rows, 128), F32),
            dma((n,)),
            dma((n,)),
            dma((2,)),
            dma((2, n)),
            dma((lines,)),
            dma((lines,)),
            dma((n, pieces)),
            dma((lines, pieces)),
            dma((lines, pieces)),
            dma((n,)),
            dma((n,)),
            dma((2,)),
            dma((2,)),
            dma((n, n)),
            dma((n, n)),
            dma((2,)),
            dma,
        ],
        compiler_params=pltpu.CompilerParams(
            collective_id=channel, has_side_effects=True, vmem_limit_bytes=67_000_000
        ),
        name=f"relay_{channel}",
    )(token_counts, tokens, norm_gain, w_in, w_out, backup_in, backup_out)


def shards(tokens, norm_gain, w_in, w_out, backup_in, backup_out, layer_group, token_counts):
    n = lax.axis_size("tensor")
    sections = lax.axis_size("section")
    layers = layer_group.shape[0]
    plans = [(lost, span) for lost in range(layers - 1) for span in range(1, layers - lost)]
    shift = layer_group - jnp.arange(layers, dtype=jnp.int32)
    span = jnp.sum(shift)
    lost = jnp.argmax(shift).astype(jnp.int32)
    index = jnp.int32(0)
    for i, plan in enumerate(plans):
        index = jnp.where((lost == plan[0]) & (span == plan[1]), i, index)
    branches = [
        functools.partial(run_plan, plan, channel, n, sections)
        for channel, plan in enumerate(plans)
    ]
    return lax.switch(
        index, branches, tokens, norm_gain, w_in, w_out, backup_in, backup_out, token_counts
    )


def solution(mesh):
    return jax.shard_map(
        shards,
        mesh=mesh,
        in_specs=(
            P(),
            P(),
            P("section", None, "tensor", None),
            P("section", "tensor", None),
            P("section", None, "tensor", None),
            P("section", None, "tensor"),
            P(),
            P(),
        ),
        out_specs=P("section", None, "tensor", None),
        check_vma=False,
    )
```

```python
import functools

import jax
import jax.numpy as jnp
from jax import lax
from jax.experimental import pallas as pl
from jax.experimental.pallas import tpu as pltpu
from jax.sharding import PartitionSpec as P

NORM_EPS = 0.25
MESH = pl.DeviceIdType.MESH
F32 = jnp.float32
BF16 = jnp.bfloat16


def as_int(condition):
    return jnp.where(condition, 1, 0)


def relay_kernel(
    cfg, counts, tokens_hbm, gain_hbm, w_in, w_out, b_in, b_out, out,
    wi, wo, xs, acc, hid, hidp, psum, rsum, ssum, res, xblk, psum2, rsum2, part_in, part_sum, part_low, row_out, row_in, tok, tsel, gain, gain_row, ssq, first_scale,
    wi_sem, wp_sem, wo_sem, in_sem, ag_recv, own_send, fwd_send, h_recv, h_own, h_fwd, h_line,
    rs_send, rs_recv, res_sem, xb_sem, rs2_send, rs2_recv, part_send, part_recv, low_send, low_recv, row_send, row_recv,
):
    lost, span, sections, layers, n, tok_rows, features, units, pieces = cfg
    half = tok_rows // 2
    rows = tok_rows + half
    share = tok_rows // n
    width = features // n
    lines = n // 2
    piece = units // pieces
    square = 256
    flip = width % square == 0 and piece == square
    group = lax.axis_index("section")
    me = lax.axis_index("tensor")
    line = me // 2
    side = lax.rem(me, 2)

    def moved(level):
        return (level >= lost) & (level < lost + span)

    def owner(level):
        return level + as_int(moved(level))

    def near(i):
        edge = jnp.minimum(line, lines - 1 - line)
        alternate = jnp.where(lax.rem(i, 2) == 1, line + (i + 1) // 2, line - i // 2)
        beyond = jnp.where(line < lines - 1 - line, i, lines - 1 - i)
        return jnp.where(i <= 2 * edge, alternate, beyond)

    def row_slot(i):
        return 2 * near(i) + side

    def across_slot(i):
        return 2 * near(i) + 1 - side

    def step_slot(s):
        across = (s == 2) | (s > lines)
        i = jnp.where(s < 2, s, jnp.where(s == 2, 0, jnp.where(s > lines, s - lines, s - 1)))
        return across, i, 2 * near(i) + jnp.where(across, 1 - side, side)

    def columns(slot):
        return pl.ds(pl.multiple_of(slot * width, 128), width)

    def load_in(src, slot):
        return pltpu.make_async_copy(src.at[0, :, :, columns(slot)], wi.at[slot], wi_sem.at[slot])

    def load_out_own(slot):
        return pltpu.make_async_copy(w_out.at[0, :, columns(slot)], wo.at[slot], wo_sem.at[slot])

    def load_out_backup(slot):
        start = pl.multiple_of(slot * units, 64)
        return pltpu.make_async_copy(b_out.at[0, pl.ds(start, units), :], wo.at[slot], wo_sem.at[slot])

    def each(count, body):
        def step(i, carry):
            body(i)
            return carry

        lax.fori_loop(0, count, step, 0)

    def start_in(src):
        each(n, lambda s: load_in(src, step_slot(s)[2]).start())

    def piece_rows(p):
        return pl.ds(pl.multiple_of(p * piece, 64), piece)

    def load_tile(src, p, slot):
        return pltpu.make_async_copy(
            src.at[0, :, piece_rows(p), columns(slot)],
            wi.at[slot, :, piece_rows(p), :],
            wp_sem.at[p, slot],
        )

    ahead = min(5, pieces)

    def start_tile(p):
        each(n, lambda c: load_tile(b_in if lost == 0 else w_in, p, c).start())

    def start_out_own():
        each(n, lambda s: load_out_own(step_slot(s)[2]).start())

    def start_out_backup():
        each(n, lambda s: load_out_backup(step_slot(s)[2]).start())

    barrier = pltpu.get_barrier_semaphore()

    def greet(o):
        target = (lax.rem(group + o // n, sections), lax.rem(me + lax.rem(o, n), n))
        pl.semaphore_signal(barrier, inc=1, device_id=target, device_id_type=MESH)

    fetch_tok = pltpu.make_async_copy(tokens_hbm, tok, in_sem.at[0])
    fetch_gain = pltpu.make_async_copy(gain_hbm, gain, in_sem.at[1])
    fetch_tok.start()
    fetch_gain.start()
    starts = group == int(lost == 0)
    has_backup = (group > lost) & (group <= lost + span)
    has_own = (group < lost) | (group >= lost + span)
    double = group == lost + span

    @pl.when(starts)
    def _():
        each(ahead, start_tile)

    @pl.when(has_backup & jnp.logical_not(starts))
    def _():
        start_in(b_in)
        start_out_backup()

    @pl.when(has_own & jnp.logical_not(has_backup) & jnp.logical_not(starts))
    def _():
        start_in(w_in)
        start_out_own()

    each(sections * n - 1, lambda o: greet(o + 1))
    fetch_tok.wait()
    fetch_gain.wait()
    full_second = counts[1] > counts[0]
    part_count = jnp.minimum(counts[0], counts[1])
    row_ids = lax.broadcasted_iota(jnp.int32, (rows, 1), 0)
    keep = ((row_ids < tok_rows) | (row_ids - tok_rows < part_count)).astype(F32)

    def pick_tokens(mb, cols):
        return jnp.where(full_second, tok[1 - mb, :, cols], tok[mb, :, cols])

    pick = (
        lax.broadcasted_iota(jnp.int32, (8, tok_rows), 1)
        == me * share + lax.broadcasted_iota(jnp.int32, (8, tok_rows), 0)
    ).astype(BF16)

    def keep_tokens(c):
        for mb in range(2):
            chosen = jnp.dot(pick, pick_tokens(mb, columns(c)), preferred_element_type=F32)
            tsel[mb, :, columns(c)] = chosen.astype(BF16)

    def add_squares(wide):
        square_sum = wide * wide
        lane = square_sum[:, :128]
        for q in range(1, width // 128):
            lane = lane + square_sum[:, q * 128 : (q + 1) * 128]
        ssq[...] += lane

    def row_scale():
        mean_square = jnp.sum(ssq[...], axis=1, keepdims=True) * (1.0 / features)
        return lax.rsqrt(mean_square + NORM_EPS)

    def activate(gate, up):
        return (gate / (1.0 + jnp.exp(-gate)) * up).astype(BF16)

    def project(lhs, weights):
        return lax.dot_general(lhs, weights, (((1,), (1,)), ((), ())), preferred_element_type=F32)

    def ready(slot):
        load_in(w_in, slot).wait()

    def turn(slot, p, halves):
        for h in halves:
            for k in range(width // square):
                at = (slot, h, piece_rows(p), slice(k * square, (k + 1) * square))
                wi[at] = wi[at].T

    ssq[...] = jnp.zeros_like(ssq)

    @pl.when(starts)
    def _():
        def enter_tokens(c):
            xs[0, c, :tok_rows] = pick_tokens(0, columns(c))
            xs[0, c, tok_rows:] = pick_tokens(1, columns(c))[:half]
            wide = xs[0, c].astype(F32)
            add_squares(wide)
            psum[c] = (wide * gain[:1, columns(c)].astype(F32)).astype(BF16)

        each(n, enter_tokens)

    @pl.when(jnp.logical_not(starts))
    def _():
        each(n, keep_tokens)

    def first_tile(p):
        each(n, lambda c: load_tile(w_in, p, c).wait())

        @pl.when(p + ahead < pieces)
        def _():
            start_tile(p + ahead)

        @pl.when(p + ahead == pieces)
        def _():
            if lost == 0:
                start_out_backup()
            else:
                start_out_own()

        sums = []
        for h in range(2):
            total = project(psum[0], wi[0, h, piece_rows(p)])
            for c in range(1, n):
                total = total + project(psum[c], wi[c, h, piece_rows(p)])
            sums.append(total * first_scale[:, :1])
        hid[me if lost == 0 else n, p] = activate(*sums)

    early = pieces if lost > 0 else min(3, pieces - 1)

    @pl.when(starts)
    def _():
        first_scale[...] = jnp.broadcast_to(row_scale(), first_scale.shape)
        each(early, first_tile)

    @pl.when((group != lost) & jnp.logical_not(starts))
    def _():
        def prepare(slot):
            ready(slot)
            if flip:
                each(pieces, lambda p: turn(slot, p, (0, 1)))

        each(n, lambda s: prepare(step_slot(s)[2]))

    pl.semaphore_wait(barrier, sections * n - 1)

    def remote(src, dst, send, recv, device):
        return pltpu.make_async_remote_copy(
            src_ref=src, dst_ref=dst, send_sem=send, recv_sem=recv, device_id=device, device_id_type=MESH
        )

    across_peer = (group, 2 * line + 1 - side)

    ends = (line == 0) | (line == lines - 1)
    far_across = (group, 2 * (lines - 1 - line) + 1 - side)

    def hops(i):
        return jnp.abs(near(i) - line)

    def ag_copy(par, slot, send, device):
        return remote(xs.at[par, slot], xs.at[par, slot], send, ag_recv.at[par, slot], device)

    def h_copy(slot, p, send, device):
        return remote(hid.at[slot, p], hid.at[slot, p], send, h_recv.at[slot, p], device)

    def rs_copy(target_group, target):
        return remote(
            psum.at[target], rsum.at[me], rs_send.at[target], rs_recv.at[me], (target_group, target)
        )

    def res_copy(par, target_group):
        return remote(xs.at[par, me], res, res_sem.at[0], res_sem.at[1], (target_group, me))

    def xb_copy(target_group):
        return remote(xblk, xblk, xb_sem.at[0], xb_sem.at[1], (target_group, me))

    upper = n // 2

    def rs2_copy(src, target, source, c, count):
        return remote(
            psum2.at[target, c, pl.ds(0, count)],
            rsum2.at[source, c, pl.ds(0, count)],
            rs2_send.at[target, c],
            rs2_recv.at[source, c],
            (group, src),
        )

    def part_copy(device, target, source, c):
        return remote(
            psum2.at[target, c, pl.ds(8, 8)],
            part_in.at[source, c],
            part_send.at[target, c],
            part_recv.at[source, c],
            (group, device),
        )

    def sum_copy(device, c):
        return remote(
            part_sum.at[c], part_low.at[c], low_send.at[c], low_recv.at[c], (group, device)
        )

    def each_row_copy(c, act):
        def plain(o):
            target = lax.rem(me + o + 1, n)

            @pl.when((me < upper) & (target < upper))
            def _():
                act(rs2_copy(target, target, me, c, 16))

            @pl.when((me >= upper) | (target >= upper))
            def _():
                act(rs2_copy(target, target, me, c, 8))

        each(n - 1, plain)

        @pl.when(me >= upper)
        def _():
            def part(o):
                target = lax.rem(me + o + 1, upper)
                act(part_copy(target + upper, target, me - upper, c))

            each(upper - 1, part)

    def beyond(i):
        rises = line > near(i)
        target = jnp.where(rises, line + 1, line - 1)
        return (target >= 0) & (target < lines), (group, 2 * target + side)

    def send_hidden(p):
        @pl.when(line < lines - 1)
        def _():
            h_copy(me, p, h_own.at[1, p], (group, me + 2)).start()

        @pl.when(line > 0)
        def _():
            h_copy(me, p, h_own.at[2, p], (group, me - 2)).start()

        h_copy(me, p, h_own.at[0, p], across_peer).start()

    def row_copy(i, target_group):
        return remote(row_out, row_in, row_send.at[i], row_recv, (target_group, me))

    def row_choice(count):
        r = lax.broadcasted_iota(jnp.int32, (16, count), 0)
        c = lax.broadcasted_iota(jnp.int32, (16, count), 1)
        inner = lax.rem(r, 8)
        row = me * share + inner
        full = (r < 8) & (c == row)
        part = (r >= 8) & (c == row + tok_rows) & (row < half)
        return ((inner < share) & (full | part)).astype(BF16)

    if lost == 0:

        @pl.when(starts)
        def _():
            each(early, send_hidden)

            def later_tile(p):
                first_tile(p + early)
                send_hidden(p + early)

            each(pieces - early, later_tile)

    def level_body(level):
        par = lax.rem(level, 2)
        home = owner(jnp.minimum(level + 1, layers - 1))
        first = level == 0
        last = level == layers - 1
        before = owner(jnp.maximum(level - 1, 0))
        is_moved = moved(level)
        before_moved = moved(level - 1)

        @pl.when(jnp.logical_not(first) & jnp.logical_not(before_moved))
        def _():
            res_copy(par, group).wait_recv()
            for j in range(n):
                remote(psum.at[0], rsum.at[j], rs_send.at[0], rs_recv.at[j], (group, me)).wait_recv()
            total = rsum[0].astype(F32)
            for j in range(1, n):
                total = total + rsum[j].astype(F32)
            xs[par, me] = (res[...].astype(F32) + keep * total).astype(BF16)

        @pl.when(jnp.logical_not(first) & before_moved)
        def _():
            @pl.when(before != group)
            def _():
                xb_copy(group).wait_recv()

            xs[par, me] = xblk[...]

        @pl.when(jnp.logical_not(first))
        def _():
            ag_copy(par, me, own_send.at[0], across_peer).start()
            each(
                lines - 1,
                lambda i: ag_copy(par, me, own_send.at[i + 1], (group, row_slot(i + 1))).start(),
            )

            @pl.when(ends)
            def _():
                ag_copy(par, me, own_send.at[lines], far_across).start()

        @pl.when(jnp.logical_not(last) & jnp.logical_not(is_moved))
        def _():
            res_copy(par, home).start()

        def chunk(s, turned):
            across, i, slot = step_slot(s)

            @pl.when(s > 0)
            def _():
                ag_copy(par, slot, own_send.at[0], across_peer).wait_recv()

            @pl.when((s > 0) & jnp.logical_not(across) & (hops(i) < lines - 1))
            def _():
                ag_copy(par, slot, fwd_send.at[i], across_peer).start()

            wide = xs[par, slot].astype(F32)
            add_squares(wide)
            scaled = (wide * gain_row[:, columns(slot)]).astype(BF16)
            for p in range(pieces):
                for h in range(2):
                    tile = wi[slot, h, p * piece : (p + 1) * piece]
                    if flip and h in turned:
                        total = acc[h, p]
                        for k in range(width // square):
                            cols = slice(k * square, (k + 1) * square)
                            total = total + jnp.dot(
                                scaled[:, cols], tile[:, cols], preferred_element_type=F32
                            )
                        acc[h, p] = total
                    else:
                        acc[h, p] += project(scaled, tile)

        @pl.when(jnp.logical_not(first))
        def _():
            acc[...] = jnp.zeros_like(acc)
            ssq[...] = jnp.zeros_like(ssq)
            for index in range(layers):

                @pl.when(level == index)
                def _():
                    gain_row[...] = gain[index : index + 1].astype(F32)

            @pl.when(before != group)
            def _():
                each(n, lambda s: chunk(s, (0, 1)))

            @pl.when(before == group)
            def _():
                each(n, lambda s: chunk(s, (1,)))

        scale = row_scale()

        def hidden(p):
            return activate(acc[0, p] * scale, acc[1, p] * scale)

        def down(source, weights):
            total = jnp.dot(source[0], wo[weights, :piece], preferred_element_type=F32)
            for p in range(1, pieces):
                total = total + jnp.dot(
                    source[p], wo[weights, p * piece : (p + 1) * piece], preferred_element_type=F32
                )
            return total

        choice = row_choice(rows)
        hand_before = jnp.logical_not(first) & (before != group)
        hand_lost = jnp.logical_not(first) & (level == lost)

        def hand_rows():
            @pl.when(hand_before | hand_lost)
            def _():
                def choose(c):
                    chosen = jnp.dot(choice, xs[par, c], preferred_element_type=F32)
                    row_out[:, columns(c)] = chosen.astype(BF16)

                each(n, choose)

            @pl.when(hand_before)
            def _():
                row_copy(0, before).start()

            @pl.when(hand_lost)
            def _():
                row_copy(1, lost).start()

        @pl.when(is_moved)
        def _():
            def produce(p):
                hid[me, p] = hidden(p)
                send_hidden(p)

            @pl.when(jnp.logical_not(first))
            def _():
                each(pieces, produce)

            @pl.when(double)
            def _():
                start_in(w_in)

            hand_rows()

            def contribution(slot):
                load_out_own(slot).wait()
                return down(hid.at[slot], slot).astype(BF16).astype(F32)

            ssum[...] = jnp.zeros_like(ssum)

            share_of_turns = -(-n // (lines - 1))

            def turn_next(turn_step):
                for t in range(share_of_turns):
                    unit = turn_step * share_of_turns + t

                    @pl.when(unit < n * pieces)
                    def _():
                        slot = step_slot(unit // pieces)[2]

                        @pl.when(lax.rem(unit, pieces) == 0)
                        def _():
                            ready(slot)

                        if flip:
                            turn(slot, lax.rem(unit, pieces), (1,))

            def gather(s):
                across, i, slot = step_slot(s)
                further, target = beyond(i)

                def pass_on(p):
                    h_copy(slot, p, h_own.at[0, p], across_peer).wait_recv()

                    @pl.when(further)
                    def _():
                        h_copy(slot, p, h_line.at[i, p], target).start()

                    h_copy(slot, p, h_fwd.at[i, p], across_peer).start()

                    @pl.when(double)
                    def _():
                        turn_next((i - 1) * pieces + p)

                @pl.when((s > 0) & jnp.logical_not(across))
                def _():
                    each(pieces, pass_on)

                @pl.when(across)
                def _():
                    each(pieces, lambda p: h_copy(slot, p, h_own.at[0, p], across_peer).wait_recv())

                ssum[...] += contribution(slot)

            each(n, gather)
            xblk[...] = (xs[par, me].astype(F32) + keep * ssum[...]).astype(BF16)

            @pl.when(home != group)
            def _():
                xb_copy(home).start()

            @pl.when(double)
            def _():
                start_out_own()

        @pl.when(jnp.logical_not(is_moved) & jnp.logical_not(last))
        def _():
            def produce(p):
                hid[n, p] = hidden(p)

            @pl.when(jnp.logical_not(first))
            def _():
                each(pieces, produce)

            def reduce_block(s):
                slot = step_slot(n - 1 - s)[2]
                load_out_own(slot).wait()
                psum[slot] = down(hid.at[n], slot).astype(BF16)
                rs_copy(home, slot).start()

            each(n, reduce_block)
            hand_rows()

        @pl.when(last)
        def _():
            r = lax.broadcasted_iota(jnp.int32, (n * 16, rows), 0)
            c = lax.broadcasted_iota(jnp.int32, (n * 16, rows), 1)
            inner = lax.rem(r, 8)
            row = (r // 16) * share + inner
            is_full = lax.rem(r, 16) < 8
            target_row = jnp.where(is_full, row, row + tok_rows)
            valid = (inner < share) & (is_full | (row < half))
            order = (valid & (c == target_row)).astype(BF16)

            def produce(p):
                hidp[p] = jnp.dot(order, hidden(p), preferred_element_type=F32).astype(BF16)

            each(pieces, produce)

            def reduce_rows(c):
                load_out_own(c).wait()
                total = down(hidp, c).astype(BF16)
                for j in range(n):
                    psum2[j, c] = total[16 * j : 16 * (j + 1)]
                rsum2[me, c] = psum2[me, c]
                each_row_copy(c, lambda copy: copy.start())

                @pl.when(me >= upper)
                def _():
                    part_in[me - upper, c] = psum2[me - upper, c, 8:]

            each(n, reduce_rows)
            hand_rows()

        @pl.when(last)
        def _():
            r = lax.broadcasted_iota(jnp.int32, (16, 1), 0)
            kept = ((r < 8) | (me * share + r - 8 < part_count)).astype(F32)

            def gather_part(c):
                def arrived(o):
                    source = lax.rem(me + o + 1, upper)
                    part_copy(me, source, source, c).wait_recv()

                each(upper - 1, arrived)
                total = part_in[0, c].astype(F32)
                for j in range(1, upper):
                    total = total + part_in[j, c].astype(F32)
                part_sum[c] = total.astype(BF16)
                sum_copy(me - upper, c).start()

            @pl.when(me >= upper)
            def _():
                each(n, gather_part)

            def finish(c):
                def arrived(o):
                    source = lax.rem(me + o + 1, n)

                    @pl.when((me < upper) & (source < upper))
                    def _():
                        rs2_copy(me, me, source, c, 16).wait_recv()

                    @pl.when((me >= upper) | (source >= upper))
                    def _():
                        rs2_copy(me, me, source, c, 8).wait_recv()

                each(n - 1, arrived)

                @pl.when(me < upper)
                def _():
                    sum_copy(me, c).wait_recv()

                full_sum = rsum2[0, c, :8].astype(F32)
                for j in range(1, n):
                    full_sum = full_sum + rsum2[j, c, :8].astype(F32)
                part_total = part_low[c].astype(F32)
                for j in range(upper):
                    part_total = part_total + rsum2[j, c, 8:].astype(F32)
                total = jnp.concatenate([full_sum, part_total], axis=0)
                entered = jnp.dot(choice, xs[par, c], preferred_element_type=F32)
                row_in[:, columns(c)] = (entered + kept * total).astype(BF16)

            each(n, finish)

        @pl.when(jnp.logical_not(first))
        def _():
            each(lines, lambda i: ag_copy(par, me, own_send.at[i], across_peer).wait_send())

            @pl.when(ends)
            def _():
                ag_copy(par, me, own_send.at[lines], far_across).wait_send()

            def forwarded(i):
                @pl.when(hops(i) < lines - 1)
                def _():
                    ag_copy(par, me, fwd_send.at[i], across_peer).wait_send()

            each(lines - 1, lambda i: forwarded(i + 1))

        @pl.when(is_moved & (home != group))
        def _():
            xb_copy(home).wait_send()

        @pl.when(jnp.logical_not(is_moved) & jnp.logical_not(last))
        def _():
            res_copy(par, home).wait_send()
            each(n, lambda s: rs_copy(home, s).wait_send())

        @pl.when(last)
        def _():
            each(n, lambda c: each_row_copy(c, lambda copy: copy.wait_send()))

            @pl.when(me >= upper)
            def _():
                each(n, lambda c: sum_copy(me, c).wait_send())

    def level(l):
        @pl.when(group == owner(l))
        def _():
            level_body(l)

    each(layers, level)

    @pl.when(starts)
    def _():
        each(n, keep_tokens)

    @pl.when(has_backup)
    def _():
        def left(p):
            h_copy(me, p, h_own.at[0, p], across_peer).wait_send()

            @pl.when(line < lines - 1)
            def _():
                h_copy(me, p, h_own.at[1, p], across_peer).wait_send()

            @pl.when(line > 0)
            def _():
                h_copy(me, p, h_own.at[2, p], across_peer).wait_send()

            def passed(i):
                h_copy(me, p, h_fwd.at[i, p], across_peer).wait_send()

                @pl.when(beyond(i)[0])
                def _():
                    h_copy(me, p, h_line.at[i, p], across_peer).wait_send()

            each(lines - 1, lambda i: passed(i + 1))

        each(pieces, left)

    @pl.when((group != lost) & jnp.logical_not(starts))
    def _():
        row_copy(0, group).wait_send()

    @pl.when((lost >= 1) & (group == lost + 1))
    def _():
        row_copy(1, group).wait_send()

    untouched = (lost == 0) & (group == 0)

    @pl.when(jnp.logical_not(untouched) & (group != sections - 1))
    def _():
        row_copy(0, group).wait_recv()

    @pl.when(untouched)
    def _():
        row_in[:8] = tsel[0]
        row_in[8:] = tsel[1]

    r = lax.broadcasted_iota(jnp.int32, (8, 1), 0)
    full_rows = row_in[:8]
    part_rows = jnp.where(me * share + r < half, row_in[8:], tsel[1])
    out[0, 0] = jnp.where(full_second, part_rows, full_rows)[:share]
    out[0, 1] = jnp.where(full_second, full_rows, part_rows)[:share]


def run_plan(
    plan, channel, n, sections, tokens, norm_gain, w_in, w_out, backup_in, backup_out, token_counts
):
    _, tok_rows, features = tokens.shape
    layers = norm_gain.shape[0]
    units = w_in.shape[2]
    piece = next((size for size in (256, 128) if units % size == 0), units)
    pieces = units // piece
    rows = tok_rows + tok_rows // 2
    width = features // n
    lines = n // 2
    cfg = plan + (sections, layers, n, tok_rows, features, units, pieces)
    anywhere = pl.BlockSpec(memory_space=pl.ANY)
    dma = pltpu.SemaphoreType.DMA
    return pl.pallas_call(
        functools.partial(relay_kernel, cfg),
        out_shape=jax.ShapeDtypeStruct((1, 2, tok_rows // n, features), BF16),
        in_specs=[pl.BlockSpec(memory_space=pltpu.SMEM)] + [anywhere] * 6,
        out_specs=pl.BlockSpec(memory_space=pltpu.VMEM),
        scratch_shapes=[
            pltpu.VMEM((n, 2, units, width), BF16),
            pltpu.VMEM((n, units, width), BF16),
            pltpu.VMEM((2, n, rows, width), BF16),
            pltpu.VMEM((2, pieces, rows, piece), F32),
            pltpu.VMEM((n + 1, pieces, rows, piece), BF16),
            pltpu.VMEM((pieces, n * 16, piece), BF16),
            pltpu.VMEM((n, rows, width), BF16),
            pltpu.VMEM((n, rows, width), BF16),
            pltpu.VMEM((rows, width), F32),
            pltpu.VMEM((rows, width), BF16),
            pltpu.VMEM((rows, width), BF16),
            pltpu.VMEM((n, n, 16, width), BF16),
            pltpu.VMEM((n, n, 16, width), BF16),
            pltpu.VMEM((n // 2, n, 8, width), BF16),
            pltpu.VMEM((n, 8, width), BF16),
            pltpu.VMEM((n, 8, width), BF16),
            pltpu.VMEM((16, features), BF16),
            pltpu.VMEM((16, features), BF16),
            pltpu.VMEM((2, tok_rows, features), BF16),
            pltpu.VMEM((2, 8, features), BF16),
            pltpu.VMEM((layers, features), BF16),
            pltpu.VMEM((1, features), F32),
            pltpu.VMEM((rows, 128), F32),
            pltpu.VMEM((rows, 128), F32),
            dma((n,)),
            dma((pieces, n)),
            dma((n,)),
            dma((2,)),
            dma((2, n)),
            dma((lines + 1,)),
            dma((lines,)),
            dma((n, pieces)),
            dma((3, pieces)),
            dma((lines, pieces)),
            dma((lines, pieces)),
            dma((n,)),
            dma((n,)),
            dma((2,)),
            dma((2,)),
            dma((n, n)),
            dma((n, n)),
            dma((n // 2, n)),
            dma((n // 2, n)),
            dma((n,)),
            dma((n,)),
            dma((2,)),
            dma,
        ],
        compiler_params=pltpu.CompilerParams(
            collective_id=channel, has_side_effects=True, vmem_limit_bytes=67_000_000
        ),
        name=f"relay_{channel}",
    )(token_counts, tokens, norm_gain, w_in, w_out, backup_in, backup_out)


def shards(tokens, norm_gain, w_in, w_out, backup_in, backup_out, layer_group, token_counts):
    n = lax.axis_size("tensor")
    sections = lax.axis_size("section")
    layers = layer_group.shape[0]
    plans = [(lost, span) for lost in range(layers - 1) for span in range(1, layers - lost)]
    code = sum((layer_group[l] - l) << l for l in range(layers))
    index = jnp.int32(0)
    for i, (lost, span) in enumerate(plans):
        index = jnp.where(code == sum(1 << l for l in range(lost, lost + span)), i, index)
    branches = [
        functools.partial(run_plan, plan, channel, n, sections)
        for channel, plan in enumerate(plans)
    ]
    return lax.switch(
        index, branches, tokens, norm_gain, w_in, w_out, backup_in, backup_out, token_counts
    )


def solution(mesh):
    return jax.shard_map(
        shards,
        mesh=mesh,
        in_specs=(
            P(),
            P(),
            P("section", None, "tensor", None),
            P("section", "tensor", None),
            P("section", None, "tensor", None),
            P("section", None, "tensor"),
            P(),
            P(),
        ),
        out_specs=P("section", None, "tensor", None),
        check_vma=False,
    )
```

```python
import functools

import jax
import jax.numpy as jnp
from jax import lax
from jax.experimental import pallas as pl
from jax.experimental.pallas import tpu as pltpu
from jax.sharding import PartitionSpec as P

NORM_EPS = 0.25
MESH = pl.DeviceIdType.MESH
F32 = jnp.float32
BF16 = jnp.bfloat16


def as_int(condition):
    return jnp.where(condition, 1, 0)


def relay_kernel(
    cfg, counts, tokens_hbm, gain_hbm, w_in, w_out, b_in, b_out, out,
    wi, wo, xs, acc, hid, hidp, psum, rsum, ssum, res, xblk, psum2, rsum2, part_in, part_sum, part_low, row_out, row_in, tok, tsel, gain, gain_row, ssq, first_scale,
    wi_sem, wp_sem, wo_sem, in_sem, ag_recv, own_send, fwd_send, h_recv, h_own, h_fwd, h_line,
    rs_send, rs_recv, res_sem, xb_sem, rs2_send, rs2_recv, part_send, part_recv, low_send, low_recv, row_send, row_recv,
):
    lost, span, sections, layers, n, tok_rows, features, units, pieces = cfg
    half = tok_rows // 2
    rows = tok_rows + half
    share = tok_rows // n
    width = features // n
    lines = n // 2
    piece = units // pieces
    square = 256
    flip = width % square == 0 and piece == square
    group = lax.axis_index("section")
    me = lax.axis_index("tensor")
    line = me // 2
    side = lax.rem(me, 2)

    def moved(level):
        return (level >= lost) & (level < lost + span)

    def owner(level):
        return level + as_int(moved(level))

    def near(i):
        edge = jnp.minimum(line, lines - 1 - line)
        alternate = jnp.where(lax.rem(i, 2) == 1, line + (i + 1) // 2, line - i // 2)
        beyond = jnp.where(line < lines - 1 - line, i, lines - 1 - i)
        return jnp.where(i <= 2 * edge, alternate, beyond)

    def row_slot(i):
        return 2 * near(i) + side

    def across_slot(i):
        return 2 * near(i) + 1 - side

    def step_slot(s):
        across = (s == 2) | (s > lines)
        i = jnp.where(s < 2, s, jnp.where(s == 2, 0, jnp.where(s > lines, s - lines, s - 1)))
        return across, i, 2 * near(i) + jnp.where(across, 1 - side, side)

    def columns(slot):
        return pl.ds(pl.multiple_of(slot * width, 128), width)

    def load_in(src, slot):
        return pltpu.make_async_copy(src.at[0, :, :, columns(slot)], wi.at[slot], wi_sem.at[slot])

    def load_out_own(slot):
        return pltpu.make_async_copy(w_out.at[0, :, columns(slot)], wo.at[slot], wo_sem.at[slot])

    def load_out_backup(slot):
        start = pl.multiple_of(slot * units, 64)
        return pltpu.make_async_copy(b_out.at[0, pl.ds(start, units), :], wo.at[slot], wo_sem.at[slot])

    def each(count, body):
        def step(i, carry):
            body(i)
            return carry

        lax.fori_loop(0, count, step, 0)

    def start_in(src):
        each(n, lambda s: load_in(src, step_slot(s)[2]).start())

    def piece_rows(p):
        return pl.ds(pl.multiple_of(p * piece, 64), piece)

    def load_tile(src, p, slot):
        return pltpu.make_async_copy(
            src.at[0, :, piece_rows(p), columns(slot)],
            wi.at[slot, :, piece_rows(p), :],
            wp_sem.at[p, slot],
        )

    ahead = min(5, pieces)

    def start_tile(p):
        each(n, lambda c: load_tile(b_in if lost == 0 else w_in, p, c).start())

    def start_out_own():
        each(n, lambda s: load_out_own(step_slot(n - 1 - s)[2]).start())

    def start_out_backup():
        each(n, lambda s: load_out_backup(step_slot(s)[2]).start())

    barrier = pltpu.get_barrier_semaphore()

    def greet(o):
        target = (lax.rem(group + o // n, sections), lax.rem(me + lax.rem(o, n), n))
        pl.semaphore_signal(barrier, inc=1, device_id=target, device_id_type=MESH)

    fetch_tok = pltpu.make_async_copy(tokens_hbm, tok, in_sem.at[0])
    fetch_gain = pltpu.make_async_copy(gain_hbm, gain, in_sem.at[1])
    fetch_tok.start()
    fetch_gain.start()
    starts = group == int(lost == 0)
    has_backup = (group > lost) & (group <= lost + span)
    has_own = (group < lost) | (group >= lost + span)
    double = group == lost + span

    @pl.when(starts)
    def _():
        each(ahead, start_tile)

    @pl.when(has_backup & jnp.logical_not(starts))
    def _():
        start_in(b_in)
        start_out_backup()

    @pl.when(has_own & jnp.logical_not(has_backup) & jnp.logical_not(starts))
    def _():
        start_in(w_in)
        start_out_own()

    each(sections * n - 1, lambda o: greet(o + 1))
    fetch_tok.wait()
    fetch_gain.wait()
    full_second = counts[1] > counts[0]
    part_count = jnp.minimum(counts[0], counts[1])
    row_ids = lax.broadcasted_iota(jnp.int32, (rows, 1), 0)
    keep = ((row_ids < tok_rows) | (row_ids - tok_rows < part_count)).astype(F32)

    def pick_tokens(mb, cols):
        return jnp.where(full_second, tok[1 - mb, :, cols], tok[mb, :, cols])

    pick = (
        lax.broadcasted_iota(jnp.int32, (8, tok_rows), 1)
        == me * share + lax.broadcasted_iota(jnp.int32, (8, tok_rows), 0)
    ).astype(BF16)

    def keep_tokens(c):
        for mb in range(2):
            chosen = jnp.dot(pick, pick_tokens(mb, columns(c)), preferred_element_type=F32)
            tsel[mb, :, columns(c)] = chosen.astype(BF16)

    def add_squares(wide):
        square_sum = wide * wide
        lane = square_sum[:, :128]
        for q in range(1, width // 128):
            lane = lane + square_sum[:, q * 128 : (q + 1) * 128]
        ssq[...] += lane

    def row_scale():
        mean_square = jnp.sum(ssq[...], axis=1, keepdims=True) * (1.0 / features)
        return lax.rsqrt(mean_square + NORM_EPS)

    def activate(gate, up):
        return (gate / (1.0 + jnp.exp(-gate)) * up).astype(BF16)

    def project(lhs, weights):
        return lax.dot_general(lhs, weights, (((1,), (1,)), ((), ())), preferred_element_type=F32)

    def ready(slot):
        load_in(w_in, slot).wait()

    def turn(slot, p, halves):
        for h in halves:
            for k in range(width // square):
                at = (slot, h, piece_rows(p), slice(k * square, (k + 1) * square))
                wi[at] = wi[at].T

    ssq[...] = jnp.zeros_like(ssq)

    @pl.when(starts)
    def _():
        def enter_tokens(c):
            xs[0, c, :tok_rows] = pick_tokens(0, columns(c))
            xs[0, c, tok_rows:] = pick_tokens(1, columns(c))[:half]
            wide = xs[0, c].astype(F32)
            add_squares(wide)
            psum[c] = (wide * gain[:1, columns(c)].astype(F32)).astype(BF16)

        each(n, enter_tokens)

    @pl.when(jnp.logical_not(starts))
    def _():
        each(n, keep_tokens)

    def first_tile(p):
        each(n, lambda c: load_tile(w_in, p, c).wait())

        @pl.when(p + ahead < pieces)
        def _():
            start_tile(p + ahead)

        @pl.when(p + ahead == pieces)
        def _():
            if lost == 0:
                start_out_backup()
            else:
                start_out_own()

        sums = []
        for h in range(2):
            total = project(psum[0], wi[0, h, piece_rows(p)])
            for c in range(1, n):
                total = total + project(psum[c], wi[c, h, piece_rows(p)])
            sums.append(total * first_scale[:, :1])
        hid[me if lost == 0 else n, p] = activate(*sums)

    early = pieces if lost > 0 else min(3, pieces - 1)

    @pl.when(starts)
    def _():
        first_scale[...] = jnp.broadcast_to(row_scale(), first_scale.shape)
        each(early, first_tile)

    @pl.when((group != lost) & jnp.logical_not(starts))
    def _():
        def prepare(slot):
            ready(slot)
            if flip:
                each(pieces, lambda p: turn(slot, p, (0, 1)))

        each(n, lambda s: prepare(step_slot(s)[2]))

    pl.semaphore_wait(barrier, sections * n - 1)

    def remote(src, dst, send, recv, device):
        return pltpu.make_async_remote_copy(
            src_ref=src, dst_ref=dst, send_sem=send, recv_sem=recv, device_id=device, device_id_type=MESH
        )

    across_peer = (group, 2 * line + 1 - side)

    ends = (line == 0) | (line == lines - 1)
    far_across = (group, 2 * (lines - 1 - line) + 1 - side)

    def hops(i):
        return jnp.abs(near(i) - line)

    def ag_copy(par, slot, send, device):
        return remote(xs.at[par, slot], xs.at[par, slot], send, ag_recv.at[par, slot], device)

    def h_copy(slot, p, send, device):
        return remote(hid.at[slot, p], hid.at[slot, p], send, h_recv.at[slot, p], device)

    def rs_copy(target_group, target):
        return remote(
            psum.at[target], rsum.at[me], rs_send.at[target], rs_recv.at[me], (target_group, target)
        )

    def res_copy(par, target_group):
        return remote(xs.at[par, me], res, res_sem.at[0], res_sem.at[1], (target_group, me))

    def xb_copy(target_group):
        return remote(xblk, xblk, xb_sem.at[0], xb_sem.at[1], (target_group, me))

    upper = n // 2

    def rs2_copy(src, target, source, c, count):
        return remote(
            psum2.at[target, c, pl.ds(0, count)],
            rsum2.at[source, c, pl.ds(0, count)],
            rs2_send.at[target, c],
            rs2_recv.at[source, c],
            (group, src),
        )

    def part_copy(device, target, source, c):
        return remote(
            psum2.at[target, c, pl.ds(8, 8)],
            part_in.at[source, c],
            part_send.at[target, c],
            part_recv.at[source, c],
            (group, device),
        )

    def sum_copy(device, c):
        return remote(
            part_sum.at[c], part_low.at[c], low_send.at[c], low_recv.at[c], (group, device)
        )

    def each_row_copy(c, act):
        def plain(o):
            target = lax.rem(me + o + 1, n)

            @pl.when((me < upper) & (target < upper))
            def _():
                act(rs2_copy(target, target, me, c, 16))

            @pl.when((me >= upper) | (target >= upper))
            def _():
                act(rs2_copy(target, target, me, c, 8))

        each(n - 1, plain)

        @pl.when(me >= upper)
        def _():
            def part(o):
                target = lax.rem(me + o + 1, upper)
                act(part_copy(target + upper, target, me - upper, c))

            each(upper - 1, part)

    def beyond(i):
        rises = line > near(i)
        target = jnp.where(rises, line + 1, line - 1)
        return (target >= 0) & (target < lines), (group, 2 * target + side)

    def send_hidden(p):
        @pl.when(line < lines - 1)
        def _():
            h_copy(me, p, h_own.at[1, p], (group, me + 2)).start()

        @pl.when(line > 0)
        def _():
            h_copy(me, p, h_own.at[2, p], (group, me - 2)).start()

        h_copy(me, p, h_own.at[0, p], across_peer).start()

    def row_copy(i, target_group):
        return remote(row_out, row_in, row_send.at[i], row_recv, (target_group, me))

    def row_choice(count):
        r = lax.broadcasted_iota(jnp.int32, (16, count), 0)
        c = lax.broadcasted_iota(jnp.int32, (16, count), 1)
        inner = lax.rem(r, 8)
        row = me * share + inner
        full = (r < 8) & (c == row)
        part = (r >= 8) & (c == row + tok_rows) & (row < half)
        return ((inner < share) & (full | part)).astype(BF16)

    if lost == 0:

        @pl.when(starts)
        def _():
            each(early, send_hidden)

            def later_tile(p):
                first_tile(p + early)
                send_hidden(p + early)

            each(pieces - early, later_tile)

    def level_body(level):
        par = lax.rem(level, 2)
        home = owner(jnp.minimum(level + 1, layers - 1))
        first = level == 0
        last = level == layers - 1
        before = owner(jnp.maximum(level - 1, 0))
        is_moved = moved(level)
        before_moved = moved(level - 1)

        @pl.when(jnp.logical_not(first) & jnp.logical_not(before_moved))
        def _():
            res_copy(par, group).wait_recv()
            for j in range(n):
                remote(psum.at[0], rsum.at[j], rs_send.at[0], rs_recv.at[j], (group, me)).wait_recv()
            total = rsum[0].astype(F32)
            for j in range(1, n):
                total = total + rsum[j].astype(F32)
            xs[par, me] = (res[...].astype(F32) + keep * total).astype(BF16)

        @pl.when(jnp.logical_not(first) & before_moved)
        def _():
            @pl.when(before != group)
            def _():
                xb_copy(group).wait_recv()

            xs[par, me] = xblk[...]

        @pl.when(jnp.logical_not(first))
        def _():
            ag_copy(par, me, own_send.at[0], across_peer).start()
            each(
                lines - 1,
                lambda i: ag_copy(par, me, own_send.at[i + 1], (group, row_slot(i + 1))).start(),
            )

            @pl.when(ends)
            def _():
                ag_copy(par, me, own_send.at[lines], far_across).start()

        @pl.when(jnp.logical_not(last) & jnp.logical_not(is_moved))
        def _():
            res_copy(par, home).start()

        def chunk(s, turned):
            across, i, slot = step_slot(s)

            @pl.when(s > 0)
            def _():
                ag_copy(par, slot, own_send.at[0], across_peer).wait_recv()

            @pl.when((s > 0) & jnp.logical_not(across) & (hops(i) < lines - 1))
            def _():
                ag_copy(par, slot, fwd_send.at[i], across_peer).start()

            wide = xs[par, slot].astype(F32)
            add_squares(wide)
            scaled = (wide * gain_row[:, columns(slot)]).astype(BF16)
            for p in range(pieces):
                for h in range(2):
                    tile = wi[slot, h, p * piece : (p + 1) * piece]
                    if flip and h in turned:
                        total = acc[h, p]
                        for k in range(width // square):
                            cols = slice(k * square, (k + 1) * square)
                            total = total + jnp.dot(
                                scaled[:, cols], tile[:, cols], preferred_element_type=F32
                            )
                        acc[h, p] = total
                    else:
                        acc[h, p] += project(scaled, tile)

        @pl.when(jnp.logical_not(first))
        def _():
            acc[...] = jnp.zeros_like(acc)
            ssq[...] = jnp.zeros_like(ssq)
            for index in range(layers):

                @pl.when(level == index)
                def _():
                    gain_row[...] = gain[index : index + 1].astype(F32)

            @pl.when(before != group)
            def _():
                each(n, lambda s: chunk(s, (0, 1)))

            @pl.when(before == group)
            def _():
                each(n, lambda s: chunk(s, (1,)))

        scale = row_scale()

        def hidden(p):
            return activate(acc[0, p] * scale, acc[1, p] * scale)

        def down(source, weights):
            total = jnp.dot(source[0], wo[weights, :piece], preferred_element_type=F32)
            for p in range(1, pieces):
                total = total + jnp.dot(
                    source[p], wo[weights, p * piece : (p + 1) * piece], preferred_element_type=F32
                )
            return total

        choice = row_choice(rows)
        hand_before = jnp.logical_not(first) & (before != group)
        hand_lost = jnp.logical_not(first) & (level == lost)

        def hand_rows():
            @pl.when(hand_before | hand_lost)
            def _():
                def choose(c):
                    chosen = jnp.dot(choice, xs[par, c], preferred_element_type=F32)
                    row_out[:, columns(c)] = chosen.astype(BF16)

                each(n, choose)

            @pl.when(hand_before)
            def _():
                row_copy(0, before).start()

            @pl.when(hand_lost)
            def _():
                row_copy(1, lost).start()

        @pl.when(is_moved)
        def _():
            def produce(p):
                hid[me, p] = hidden(p)
                send_hidden(p)

            @pl.when(jnp.logical_not(first))
            def _():
                each(pieces, produce)

            @pl.when(double)
            def _():
                start_in(w_in)

            hand_rows()

            def contribution(slot):
                load_out_own(slot).wait()
                return down(hid.at[slot], slot).astype(BF16).astype(F32)

            ssum[...] = jnp.zeros_like(ssum)

            share_of_turns = -(-n // (lines - 1))

            def turn_next(turn_step):
                for t in range(share_of_turns):
                    unit = turn_step * share_of_turns + t

                    @pl.when(unit < n * pieces)
                    def _():
                        slot = step_slot(unit // pieces)[2]

                        @pl.when(lax.rem(unit, pieces) == 0)
                        def _():
                            ready(slot)

                        if flip:
                            turn(slot, lax.rem(unit, pieces), (1,))

            def gather(s):
                across, i, slot = step_slot(s)
                further, target = beyond(i)

                def pass_on(p):
                    h_copy(slot, p, h_own.at[0, p], across_peer).wait_recv()

                    @pl.when(further)
                    def _():
                        h_copy(slot, p, h_line.at[i, p], target).start()

                    h_copy(slot, p, h_fwd.at[i, p], across_peer).start()

                    @pl.when(double)
                    def _():
                        turn_next((i - 1) * pieces + p)

                @pl.when((s > 0) & jnp.logical_not(across))
                def _():
                    each(pieces, pass_on)

                @pl.when(across)
                def _():
                    each(pieces, lambda p: h_copy(slot, p, h_own.at[0, p], across_peer).wait_recv())

                ssum[...] += contribution(slot)

            each(n, gather)
            xblk[...] = (xs[par, me].astype(F32) + keep * ssum[...]).astype(BF16)

            @pl.when(home != group)
            def _():
                xb_copy(home).start()

            @pl.when(double)
            def _():
                start_out_own()

        @pl.when(jnp.logical_not(is_moved) & jnp.logical_not(last))
        def _():
            def produce(p):
                hid[n, p] = hidden(p)

            @pl.when(jnp.logical_not(first))
            def _():
                each(pieces, produce)

            def reduce_block(s):
                slot = step_slot(n - 1 - s)[2]
                load_out_own(slot).wait()
                psum[slot] = down(hid.at[n], slot).astype(BF16)
                rs_copy(home, slot).start()

            each(n, reduce_block)
            hand_rows()

        @pl.when(last)
        def _():
            r = lax.broadcasted_iota(jnp.int32, (n * 16, rows), 0)
            c = lax.broadcasted_iota(jnp.int32, (n * 16, rows), 1)
            inner = lax.rem(r, 8)
            row = (r // 16) * share + inner
            is_full = lax.rem(r, 16) < 8
            target_row = jnp.where(is_full, row, row + tok_rows)
            valid = (inner < share) & (is_full | (row < half))
            order = (valid & (c == target_row)).astype(BF16)

            def produce(p):
                hidp[p] = jnp.dot(order, hidden(p), preferred_element_type=F32).astype(BF16)

            each(pieces, produce)

            def reduce_rows(c):
                load_out_own(c).wait()
                total = down(hidp, c).astype(BF16)
                for j in range(n):
                    psum2[j, c] = total[16 * j : 16 * (j + 1)]
                rsum2[me, c] = psum2[me, c]
                each_row_copy(c, lambda copy: copy.start())

                @pl.when(me >= upper)
                def _():
                    part_in[me - upper, c] = psum2[me - upper, c, 8:]

            each(n, reduce_rows)
            hand_rows()

        @pl.when(last)
        def _():
            r = lax.broadcasted_iota(jnp.int32, (16, 1), 0)
            kept = ((r < 8) | (me * share + r - 8 < part_count)).astype(F32)

            def gather_part(c):
                def arrived(o):
                    source = lax.rem(me + o + 1, upper)
                    part_copy(me, source, source, c).wait_recv()

                each(upper - 1, arrived)
                total = part_in[0, c].astype(F32)
                for j in range(1, upper):
                    total = total + part_in[j, c].astype(F32)
                part_sum[c] = total.astype(BF16)
                sum_copy(me - upper, c).start()

            @pl.when(me >= upper)
            def _():
                each(n, gather_part)

            def finish(c):
                each_row_copy(c, lambda copy: copy.wait_send())

                def arrived(o):
                    source = lax.rem(me + o + 1, n)

                    @pl.when((me < upper) & (source < upper))
                    def _():
                        rs2_copy(me, me, source, c, 16).wait_recv()

                    @pl.when((me >= upper) | (source >= upper))
                    def _():
                        rs2_copy(me, me, source, c, 8).wait_recv()

                each(n - 1, arrived)

                @pl.when(me < upper)
                def _():
                    sum_copy(me, c).wait_recv()

                full_sum = rsum2[0, c, :8].astype(F32)
                for j in range(1, n):
                    full_sum = full_sum + rsum2[j, c, :8].astype(F32)
                part_total = part_low[c].astype(F32)
                for j in range(upper):
                    part_total = part_total + rsum2[j, c, 8:].astype(F32)
                total = jnp.concatenate([full_sum, part_total], axis=0)
                entered = jnp.dot(choice, xs[par, c], preferred_element_type=F32)
                row_in[:, columns(c)] = (entered + kept * total).astype(BF16)

            each(n, finish)

        @pl.when(jnp.logical_not(first))
        def _():
            each(lines, lambda i: ag_copy(par, me, own_send.at[i], across_peer).wait_send())

            @pl.when(ends)
            def _():
                ag_copy(par, me, own_send.at[lines], far_across).wait_send()

            def forwarded(i):
                @pl.when(hops(i) < lines - 1)
                def _():
                    ag_copy(par, me, fwd_send.at[i], across_peer).wait_send()

            each(lines - 1, lambda i: forwarded(i + 1))

        @pl.when(is_moved & (home != group))
        def _():
            xb_copy(home).wait_send()

        @pl.when(jnp.logical_not(is_moved) & jnp.logical_not(last))
        def _():
            res_copy(par, home).wait_send()
            each(n, lambda s: rs_copy(home, s).wait_send())

        @pl.when(last)
        def _():
            @pl.when(me >= upper)
            def _():
                each(n, lambda c: sum_copy(me, c).wait_send())

    def level(l):
        @pl.when(group == owner(l))
        def _():
            level_body(l)

    each(layers, level)

    @pl.when(starts)
    def _():
        each(n, keep_tokens)

    @pl.when(has_backup)
    def _():
        def left(p):
            h_copy(me, p, h_own.at[0, p], across_peer).wait_send()

            @pl.when(line < lines - 1)
            def _():
                h_copy(me, p, h_own.at[1, p], across_peer).wait_send()

            @pl.when(line > 0)
            def _():
                h_copy(me, p, h_own.at[2, p], across_peer).wait_send()

            def passed(i):
                h_copy(me, p, h_fwd.at[i, p], across_peer).wait_send()

                @pl.when(beyond(i)[0])
                def _():
                    h_copy(me, p, h_line.at[i, p], across_peer).wait_send()

            each(lines - 1, lambda i: passed(i + 1))

        each(pieces, left)

    @pl.when((group != lost) & jnp.logical_not(starts))
    def _():
        row_copy(0, group).wait_send()

    @pl.when((lost >= 1) & (group == lost + 1))
    def _():
        row_copy(1, group).wait_send()

    untouched = (lost == 0) & (group == 0)

    @pl.when(jnp.logical_not(untouched) & (group != sections - 1))
    def _():
        row_copy(0, group).wait_recv()

    @pl.when(untouched)
    def _():
        row_in[:8] = tsel[0]
        row_in[8:] = tsel[1]

    r = lax.broadcasted_iota(jnp.int32, (8, 1), 0)
    full_rows = row_in[:8]
    part_rows = jnp.where(me * share + r < half, row_in[8:], tsel[1])
    out[0, 0] = jnp.where(full_second, part_rows, full_rows)[:share]
    out[0, 1] = jnp.where(full_second, full_rows, part_rows)[:share]


def run_plan(
    plan, channel, n, sections, tokens, norm_gain, w_in, w_out, backup_in, backup_out, token_counts
):
    _, tok_rows, features = tokens.shape
    layers = norm_gain.shape[0]
    units = w_in.shape[2]
    piece = next((size for size in (256, 128) if units % size == 0), units)
    pieces = units // piece
    rows = tok_rows + tok_rows // 2
    width = features // n
    lines = n // 2
    cfg = plan + (sections, layers, n, tok_rows, features, units, pieces)
    anywhere = pl.BlockSpec(memory_space=pl.ANY)
    dma = pltpu.SemaphoreType.DMA
    return pl.pallas_call(
        functools.partial(relay_kernel, cfg),
        out_shape=jax.ShapeDtypeStruct((1, 2, tok_rows // n, features), BF16),
        in_specs=[pl.BlockSpec(memory_space=pltpu.SMEM)] + [anywhere] * 6,
        out_specs=pl.BlockSpec(memory_space=pltpu.VMEM),
        scratch_shapes=[
            pltpu.VMEM((n, 2, units, width), BF16),
            pltpu.VMEM((n, units, width), BF16),
            pltpu.VMEM((2, n, rows, width), BF16),
            pltpu.VMEM((2, pieces, rows, piece), F32),
            pltpu.VMEM((n + 1, pieces, rows, piece), BF16),
            pltpu.VMEM((pieces, n * 16, piece), BF16),
            pltpu.VMEM((n, rows, width), BF16),
            pltpu.VMEM((n, rows, width), BF16),
            pltpu.VMEM((rows, width), F32),
            pltpu.VMEM((rows, width), BF16),
            pltpu.VMEM((rows, width), BF16),
            pltpu.VMEM((n, n, 16, width), BF16),
            pltpu.VMEM((n, n, 16, width), BF16),
            pltpu.VMEM((n // 2, n, 8, width), BF16),
            pltpu.VMEM((n, 8, width), BF16),
            pltpu.VMEM((n, 8, width), BF16),
            pltpu.VMEM((16, features), BF16),
            pltpu.VMEM((16, features), BF16),
            pltpu.VMEM((2, tok_rows, features), BF16),
            pltpu.VMEM((2, 8, features), BF16),
            pltpu.VMEM((layers, features), BF16),
            pltpu.VMEM((1, features), F32),
            pltpu.VMEM((rows, 128), F32),
            pltpu.VMEM((rows, 128), F32),
            dma((n,)),
            dma((pieces, n)),
            dma((n,)),
            dma((2,)),
            dma((2, n)),
            dma((lines + 1,)),
            dma((lines,)),
            dma((n, pieces)),
            dma((3, pieces)),
            dma((lines, pieces)),
            dma((lines, pieces)),
            dma((n,)),
            dma((n,)),
            dma((2,)),
            dma((2,)),
            dma((n, n)),
            dma((n, n)),
            dma((n // 2, n)),
            dma((n // 2, n)),
            dma((n,)),
            dma((n,)),
            dma((2,)),
            dma,
        ],
        compiler_params=pltpu.CompilerParams(
            collective_id=channel, has_side_effects=True, vmem_limit_bytes=67_000_000
        ),
        name=f"relay_{channel}",
    )(token_counts, tokens, norm_gain, w_in, w_out, backup_in, backup_out)


def shards(tokens, norm_gain, w_in, w_out, backup_in, backup_out, layer_group, token_counts):
    n = lax.axis_size("tensor")
    sections = lax.axis_size("section")
    layers = layer_group.shape[0]
    plans = [(lost, span) for lost in range(layers - 1) for span in range(1, layers - lost)]
    code = sum((layer_group[l] - l) << l for l in range(layers))
    index = jnp.int32(0)
    for i, (lost, span) in enumerate(plans):
        index = jnp.where(code == sum(1 << l for l in range(lost, lost + span)), i, index)
    branches = [
        functools.partial(run_plan, plan, channel, n, sections)
        for channel, plan in enumerate(plans)
    ]
    return lax.switch(
        index, branches, tokens, norm_gain, w_in, w_out, backup_in, backup_out, token_counts
    )


def solution(mesh):
    return jax.shard_map(
        shards,
        mesh=mesh,
        in_specs=(
            P(),
            P(),
            P("section", None, "tensor", None),
            P("section", "tensor", None),
            P("section", None, "tensor", None),
            P("section", None, "tensor"),
            P(),
            P(),
        ),
        out_specs=P("section", None, "tensor", None),
        check_vma=False,
    )
```
